32 devices in a mesh: gx: 8 (over z, y), gy: 4 (over x, core).
Axes of the slice: x: 2, y: 2, z: 4, core: 2. Of those that a mesh axis runs over, the one named last changes fastest.
Arguments:
- hidden: bfloat16 [4096, 14336], P('gx', 'gy'), may hold values from -6 to 6
- weight: bfloat16 [4096, 14336], P(None, 'gy'), may hold values from -0.0625 to 0.0625
- cotangent: bfloat16 [4096, 4096], P('gx', 'gy'), may hold values from -6 to 6
Outputs:
- output: bfloat16 [4096, 4096], P('gx', 'gy')
- hidden_grad: bfloat16 [4096, 14336], P('gx', 'gy')
- weight_grad: float32 [4096, 14336], P('gx', 'gy')
The draws below stay inside these ranges and needn't reach their ends.
All inputs are finite; a program needn't handle non-finite values.
Results may differ from the reference program's by a relative error of at most 0.001.
Values may be sent and summed in bfloat16 or wider, within the bound.
A program may use at most 128 MiB of HBM per device.

```python
import jax
import jax.numpy as jnp

D = 4096
FF = 14336
TOKENS = 4096


def strengthened(values, rng, source, target, blocks, factor):
    def block_of(position):
        return (jnp.arange(values.shape[position]) // (values.shape[position] // blocks)).reshape((-1,) + (1,) * (values.ndim - 1 - position))

    near = jax.random.permutation(rng, blocks)[block_of(target)]
    far = (block_of(target) + blocks // 2) % blocks
    return jnp.where((block_of(source) == near) | (block_of(source) == far), factor * values, values)


def block_scale(rng, dims, pieces, smallest, high):
    gain, own = 1.0, jax.random.fold_in(rng, 6)
    for position, blocks in pieces:
        heights = jnp.exp(jax.random.uniform(jax.random.fold_in(own, position), (blocks,), jnp.float32, smallest / len(pieces), high / len(pieces)))
        gain = gain * jnp.repeat(heights, dims[position] // blocks).reshape([-1 if axis == position else 1 for axis in range(len(dims))])
    return gain


def scatter_about(own_key, dims, spread, limit, shards=(), held_as=jnp.bfloat16):
    loudness = block_scale(own_key, dims, shards, -0.22, 0.18) if shards else 1.0
    values = jax.random.normal(own_key, dims, jnp.float32) * spread * loudness
    return jnp.minimum(jnp.maximum(values, -limit), limit).astype(held_as)


def gaussian_with(stream_key, shape, deviation, reach, split, heavy, kind=jnp.bfloat16):
    result = deviation * jax.random.normal(stream_key, shape, jnp.float32)
    if split:
        result = result * block_scale(stream_key, shape, split, -0.22, 0.18)
    return jnp.clip(strengthened(result, jax.random.fold_in(stream_key, 3), *heavy), -reach, reach).astype(kind)


def setup_inputs(seed: int = 0) -> dict:
    arg_keys = jax.random.split(jax.random.key(seed), 4)
    hidden = scatter_about(arg_keys[0], (TOKENS, FF), 1.0, 6.0, ((0, 8), (1, 4)))
    weight = gaussian_with(arg_keys[1], (D, FF), FF ** -0.5, 0.0625, ((1, 4),), (1, 0, 4, 2.0))
    cotangent = gaussian_with(arg_keys[2], (TOKENS, D), 1.0, 6.0, ((0, 8), (1, 4)), (0, 1, 8, 2.0))
    return {"hidden": hidden, "weight": weight, "cotangent": cotangent}


def reference(hidden, weight, cotangent):
    hidden_f = hidden.astype(jnp.float32)
    weight_f = weight.astype(jnp.float32)
    cotangent_f = cotangent.astype(jnp.float32)
    output = jnp.dot(hidden_f, weight_f.T, preferred_element_type=jnp.float32).astype(jnp.bfloat16)
    hidden_grad = jnp.dot(cotangent_f, weight_f, preferred_element_type=jnp.float32).astype(jnp.bfloat16)
    weight_grad = jnp.dot(cotangent_f.T, hidden_f, preferred_element_type=jnp.float32) * (TOKENS ** -0.5)
    return output, hidden_grad, weight_grad
```

```python
import jax
import jax.numpy as jnp
from jax import lax
from jax.sharding import PartitionSpec as P


PAIR = 2
STREAMS = 4
LANES = 128


def cuts(width, pieces):
    units = width // LANES if width % LANES == 0 else width
    step = width // units
    pieces = min(pieces, units)
    edges = [units * i // pieces * step for i in range(pieces + 1)]
    return list(zip(edges[:-1], edges[1:]))


def dot_t(a, b):
    return lax.dot_general(a, b, (((0,), (0,)), ((), ())), preferred_element_type=jnp.float32)


def shards(hidden, weight, cotangent):
    gx, gy = lax.axis_size("gx"), lax.axis_size("gy")
    nz, nx = gx // PAIR, gy // PAIR
    ix, iy = lax.axis_index("gx"), lax.axis_index("gy")
    z, y = ix // PAIR, ix % PAIR
    x, core = iy // PAIR, iy % PAIR
    rows, width = hidden.shape
    block = cotangent.shape[1]
    features = weight.shape[0]
    grad_scale = float(rows * gx) ** (-0.5)
    f32 = jnp.float32

    def z_shift(v, d):
        return lax.ppermute(v, "gx", [(g, (g + PAIR * d) % gx) for g in range(gx)])

    def y_swap(v):
        return lax.ppermute(v, "gx", [(g, g ^ 1) for g in range(gx)])

    def x_shift(v, d):
        return lax.ppermute(v, "gy", [(j, (j + PAIR * d) % gy) for j in range(gy)])

    def core_swap(v):
        return lax.ppermute(v, "gy", [(j, j ^ 1) for j in range(gy)])

    mine = jnp.stack([cotangent] + [x_shift(cotangent, d) for d in range(1, nx)])
    theirs = core_swap(mine)
    full = jnp.zeros((rows, features), cotangent.dtype)
    for d in range(nx):
        source = (x - d) % nx * PAIR
        full = lax.dynamic_update_slice(full, mine[d], (0, (source + core) * block))
        full = lax.dynamic_update_slice(full, theirs[d], (0, (source + 1 - core) * block))

    span = features // nz
    half = rows // PAIR
    fetched = jnp.stack(
        [
            z_shift(
                lax.dynamic_slice(full, (core * half, (z + t) % nz * span), (half, span)), t
            )
            for t in range(1, nz)
        ]
    )
    other = core_swap(fetched)
    low = jnp.where(core == 0, fetched, other)
    high = jnp.where(core == 0, other, fetched)
    by_shift = [lax.dynamic_slice(full, (0, z * span), (rows, span))]
    by_shift += [jnp.concatenate([low[t], high[t]]) for t in range(nz - 1)]
    rows_out = span // PAIR

    def of_feature_block(stack, which):
        return lax.dynamic_slice(stack, (0, which * rows_out), (rows * nz, rows_out))

    stacks = (
        jnp.concatenate(by_shift),
        jnp.concatenate([by_shift[-t % nz] for t in range(nz)]),
    )
    own = [of_feature_block(s, y) for s in stacks]
    peer = [of_feature_block(s, 1 - y) for s in stacks]

    partial = lax.dot_general(
        hidden, weight, (((1,), (1,)), ((), ())), preferred_element_type=f32
    )

    def columns(which_core):
        return jnp.stack(
            [
                lax.dynamic_slice(
                    partial, (0, ((x + d) % nx * PAIR + which_core) * block), (rows, block)
                )
                for d in range(nx)
            ]
        )

    chip_sum = columns(core) + core_swap(columns(1 - core))
    total = chip_sum[0]
    for d in range(1, nx):
        total = total + x_shift(chip_sum[d], d)
    output = total.astype(jnp.bfloat16)

    hidden_grad = jnp.dot(full, weight, preferred_element_type=f32).astype(jnp.bfloat16)

    weight_grad = jnp.zeros((rows_out, width), f32)
    for s, (start, stop) in enumerate(cuts(width, STREAMS)):
        way = 1 if s % 2 == 0 else -1
        held = [hidden[:, start:stop]]
        for _ in range(nz - 1):
            held.append(z_shift(held[-1], way))
        tokens = jnp.concatenate(held)
        arrived = y_swap(dot_t(peer[s % 2], tokens))
        summed = dot_t(own[s % 2], tokens) + arrived
        weight_grad = lax.dynamic_update_slice(weight_grad, summed * grad_scale, (0, start))
    return (output, hidden_grad, weight_grad)


def solution(mesh):
    return jax.shard_map(
        shards,
        mesh=mesh,
        in_specs=(P("gx", "gy"), P(None, "gy"), P("gx", "gy")),
        out_specs=(P("gx", "gy"), P("gx", "gy"), P("gx", "gy")),
        check_vma=False,
    )
```
